32 devices in a mesh: section: 2 (over y), shard: 16 (over z, x, core).
Axes of the slice: x: 2, y: 2, z: 4, core: 2. Of those that a mesh axis runs over, the one named last changes fastest.
Arguments:
- section_input: bfloat16 [4, 16, 196, 256], P(None, 'shard'), may hold values from -6 to 6
- conv_one: bfloat16 [2, 2304, 256], P('section'), may hold values from -0.125 to 0.125
- conv_two: bfloat16 [2, 2304, 256], P('section'), may hold values from -0.125 to 0.125
- unit_gain: float32 [2, 256], P('section'), may hold values from 0.5 to 1.5
- offset_bias: float32 [2, 256], P('section'), may hold values from -3 to 3
- leak_slope: float32 [2, 256], P('section'), may hold values from 0.1 to 0.4
- depthwise: bfloat16 [196, 256], replicated, may hold values from -0.4375 to 0.4375
- embed_weight: bfloat16 [256, 512], replicated, may hold values from -0.375 to 0.375
- class_centers: bfloat16 [26624, 512], P('shard'), may hold values from -6 to 6
- labels: int32 [4, 16], replicated, may hold values from 0 to 26623
- class_offsets: int32 [16], P('shard'), may hold values from 0 to 24960, as said below
Outputs:
- section_grads: bfloat16 [2, 4, 16, 196, 256], P('section', None, 'shard')
The draws below stay inside these ranges and needn't reach their ends.
Inputs may be any that keep to these rules, and one draw needn't show every extreme that they name: `class_offsets`: each entry is 1664 times a different number of 0 to 15, so the blocks of class_centers hold every class of 0 to 26623 once.
All inputs are finite; a program needn't handle non-finite values.
Results may differ from the reference program's by a relative error of at most 0.03.
Values may be sent and summed in bfloat16 or wider, within the bound.
A program may use at most 64 MiB of HBM per device.

```python
import math
import jax
import jax.numpy as jnp
from jax import lax

C = 256
EMB = 512
SIDE = 14
CLS_DEV = 1664
MICRO = 4
FACES = 16
CLASSES = 26624
N_SECTION = 2
N_SHARD = 16


def draw_class_offsets(key, part):
    order = jax.random.permutation(jax.random.fold_in(key, 17), N_SHARD)
    return (order * CLS_DEV).astype(jnp.int32)


def plant(entries, own_key, low, top_value):
    longest = entries.shape.index(max(entries.shape))
    spots = []
    for shift in (0, 1):
        where = [jax.random.randint(jax.random.fold_in(own_key, axis), (), 0, length) for axis, length in enumerate(entries.shape)]
        where[longest] = (where[longest] + shift) % entries.shape[longest]
        spots.append(tuple(where))
    return entries.at[spots[0]].set(low).at[spots[1]].set(top_value)


def levels(own_key, extent, cuts, low, largest):
    def one(position, shards_of):
        draws = jax.random.uniform(jax.random.fold_in(jax.random.fold_in(own_key, 6), position), (shards_of,), jnp.float32, low / len(cuts), largest / len(cuts))
        return jnp.repeat(jnp.exp(draws), extent[position] // shards_of).reshape((-1,) + (1,) * (len(extent) - position - 1))

    gain = one(*cuts[0])
    for cut in cuts[1:]:
        gain = gain * one(*cut)
    return gain


def scatter_about(stream_key, extent, deviation, most, split=(), kind=jnp.bfloat16):
    factor_of = levels(stream_key, extent, split, -0.22, 0.18) if split else 1.0
    values = jax.random.normal(stream_key, extent, jnp.float32) * deviation * factor_of
    return jnp.minimum(jnp.maximum(values, -most), most).astype(kind)


def setup_inputs(seed: int = 0) -> dict:
    key_of = jax.random.split(jax.random.key(seed), 12)
    return {
        "section_input": scatter_about(key_of[0], (MICRO, FACES, SIDE * SIDE, C), 1.0, 6.0, ((1, 16),)),
        "conv_one": scatter_about(key_of[1], (N_SECTION, 9 * C, C), (9 * C) ** -0.5, 0.125, ((0, 2),)),
        "conv_two": scatter_about(key_of[2], (N_SECTION, 9 * C, C), (9 * C) ** -0.5, 0.125, ((0, 2),)),
        "unit_gain": jnp.clip(1.0 + 0.1 * jax.random.normal(key_of[3], (N_SECTION, C), jnp.float32), 0.5, 1.5),
        "offset_bias": scatter_about(key_of[4], (N_SECTION, C), 0.5, 3.0, ((0, 2),), jnp.float32),
        "leak_slope": jnp.clip(0.1 + 0.3 * jax.random.uniform(key_of[5], (N_SECTION, C), jnp.float32) ** levels(key_of[5], (N_SECTION, C), ((0, 2),), -0.2, 0.2), 0.1, 0.4),
        "depthwise": scatter_about(key_of[6], (SIDE * SIDE, C), (SIDE * SIDE) ** -0.5, 0.4375),
        "embed_weight": scatter_about(key_of[7], (C, EMB), C ** -0.5, 0.375),
        "class_centers": scatter_about(key_of[8], (CLASSES, EMB), 1.0, 6.0, ((0, 16),)),
        "labels": plant(jax.random.randint(key_of[9], (MICRO, FACES), 0, CLASSES), jax.random.fold_in(key_of[9], 1), 0, CLASSES - 1).astype(jnp.int32),
        "class_offsets": draw_class_offsets(jax.random.fold_in(key_of[11], 71), 0),
    }


margin_value = 0.4
scale_value = 64.0
tiny_value = 1e-06

def conv_apply(images, weights):
    image_count = images.shape[0]
    channels = images.shape[-1]
    image_grid = images.reshape(image_count, SIDE, SIDE, channels)
    padded = jnp.pad(image_grid, ((0, 0), (1, 1), (1, 1), (0, 0)))
    pieces = [padded[:, row_shift:row_shift + SIDE, col_shift:col_shift + SIDE, :] for row_shift in range(3) for col_shift in range(3)]
    columns = jnp.concatenate(pieces, axis=3).reshape(image_count * SIDE * SIDE, 9 * channels)
    result = jnp.dot(columns, weights, preferred_element_type=jnp.float32)
    return result.reshape(image_count, SIDE * SIDE, weights.shape[1])

def flip_weights(weights):
    channels = weights.shape[1]
    tap_blocks = weights.reshape(9, channels, channels)
    return jnp.swapaxes(tap_blocks[::-1], 1, 2).reshape(9 * channels, channels)

def smooth_active(pre_active, leak):
    return leak * pre_active + (1.0 - leak) * jax.nn.softplus(4.0 * pre_active) / 4.0

def smooth_slope(pre_active, leak):
    return leak + (1.0 - leak) * jax.nn.sigmoid(4.0 * pre_active)

def unit_forward(images, first_weight, second_weight, gain_row, bias_row, leak_row):
    hidden = conv_apply(images, first_weight)
    pre_active = hidden * gain_row + bias_row
    active = smooth_active(pre_active, leak_row).astype(jnp.bfloat16)
    output = (images.astype(jnp.float32) + conv_apply(active, second_weight)).astype(jnp.bfloat16)
    return (output, pre_active)

def unit_backward(grad_out, pre_active, first_flip, second_flip, gain_row, leak_row):
    grad_active = conv_apply(grad_out, second_flip)
    grad_hidden = (grad_active * smooth_slope(pre_active, leak_row) * gain_row).astype(jnp.bfloat16)
    return (grad_out.astype(jnp.float32) + conv_apply(grad_hidden, first_flip)).astype(jnp.bfloat16)

def unit_scale(values):
    squares = lax.optimization_barrier(jnp.mean(values * values, axis=-1, keepdims=True))
    factor = lax.rsqrt(squares + tiny_value) / math.sqrt(values.shape[-1])
    return (values * factor, squares, factor)

def reference(section_input, conv_one, conv_two, unit_gain, offset_bias, leak_slope, depthwise, embed_weight, class_centers, labels, class_offsets):
    row_count = MICRO * FACES
    current = section_input.reshape(row_count, SIDE * SIDE, C)
    pre_list = []
    for section_index in range(N_SECTION):
        current, pre_active = unit_forward(current, conv_one[section_index], conv_two[section_index], unit_gain[section_index], offset_bias[section_index], leak_slope[section_index])
        pre_list.append(pre_active)
    pooled = jnp.einsum('rpc,pc->rc', current.astype(jnp.float32), depthwise.astype(jnp.float32)).astype(jnp.bfloat16)
    embedded = jnp.dot(pooled, embed_weight, preferred_element_type=jnp.float32)
    normed, squares, factor = unit_scale(embedded)
    unit_half = normed.astype(jnp.bfloat16)
    flat_labels = labels.reshape(row_count)
    blocks = class_centers.reshape(N_SHARD, CLS_DEV, EMB)

    def one_block(running, inputs):
        center_block, class_base = inputs
        centres_unit = unit_scale(center_block.astype(jnp.float32))[0].astype(jnp.bfloat16)
        cosines = jnp.dot(unit_half, centres_unit.T, preferred_element_type=jnp.float32)
        class_ids = class_base + jnp.arange(CLS_DEV, dtype=jnp.int32)
        label_hits = flat_labels[:, None] == class_ids[None, :]
        logits = scale_value * (cosines - margin_value * label_hits.astype(jnp.float32))
        exp_logits = jnp.exp(logits)
        weighted = jnp.dot(exp_logits.astype(jnp.bfloat16), centres_unit, preferred_element_type=jnp.float32)
        chosen = jnp.dot(label_hits.astype(jnp.bfloat16), centres_unit, preferred_element_type=jnp.float32)
        return ((running[0] + weighted, running[1] + chosen, running[2] + lax.optimization_barrier(jnp.sum(exp_logits, axis=1))), None)
    start_sums = (jnp.zeros((row_count, EMB), jnp.float32), jnp.zeros((row_count, EMB), jnp.float32), jnp.zeros((row_count,), jnp.float32))
    sums_out = lax.scan(one_block, start_sums, (blocks, class_offsets.astype(jnp.int32)))[0]
    grad_unit = scale_value * (sums_out[0] / sums_out[2][:, None] - sums_out[1])
    inner = lax.optimization_barrier(jnp.sum(embedded * grad_unit, axis=-1, keepdims=True))
    grad_embed = factor * (grad_unit - embedded * inner / (EMB * (squares + tiny_value)))
    grad_pooled = jnp.dot(grad_embed.astype(jnp.bfloat16), embed_weight.T, preferred_element_type=jnp.float32)
    current_grad = (grad_pooled[:, None, :] * depthwise.astype(jnp.float32)[None, :, :]).astype(jnp.bfloat16)
    grad_list = [None] * N_SECTION
    for section_index in reversed(range(N_SECTION)):
        current_grad = unit_backward(current_grad, pre_list[section_index], flip_weights(conv_one[section_index]), flip_weights(conv_two[section_index]), unit_gain[section_index], leak_slope[section_index])
        grad_list[section_index] = current_grad
    return jnp.stack(grad_list).reshape(N_SECTION, MICRO, FACES, SIDE * SIDE, C)
```

```python
import functools
import math

import jax
import jax.numpy as jnp
from jax import lax
from jax.experimental import pallas as pl
from jax.experimental.pallas import tpu as pltpu
from jax.sharding import PartitionSpec as P

MESH = pl.DeviceIdType.MESH
STRIDE = 16
ROW_BITS = 4
HALF_ROWS = 16
LANES = 128

margin_value = 0.4
scale_value = 64.0
tiny_value = 1e-06

f32 = jnp.float32
bf16 = jnp.bfloat16


def dot(left, right):
    return jnp.dot(left, right, preferred_element_type=f32)


def dot_nt(left, right):
    return lax.dot_general(left, right, (((1,), (1,)), ((), ())), preferred_element_type=f32)


def kernel(
    sections,
    shards,
    images,
    side,
    x_hbm,
    w1_hbm,
    w2_hbm,
    gain_ref,
    bias_ref,
    leak_ref,
    depth_ref,
    embed_hbm,
    centre_hbm,
    labels_ref,
    offset_ref,
    out_hbm,
    xin,
    xsend,
    gin,
    gout,
    w1,
    w2,
    w1t,
    w2t,
    embed,
    raw,
    centres,
    cols_a,
    cols_b,
    expand,
    compact,
    dw16,
    slope,
    g16,
    pooled,
    emb,
    gpool,
    unit_src,
    unit_all,
    flat,
    wide,
    label_col,
    chosen_src,
    chosen_rcv,
    part_src,
    part_rcv,
    in_sem,
    x_sem,
    xs_send,
    xs_recv,
    gs_send,
    gs_recv,
    out_sem,
    peer_send,
    peer_recv,
):
    section = lax.axis_index("section")
    me = lax.axis_index("shard")
    first = section == 0
    last = section == sections - 1
    positions = side * side
    rows = side * STRIDE
    channels = w1.shape[1]
    width = embed.shape[1]
    class_count = centres.shape[0]
    faces = shards * images

    w1_copy = pltpu.make_async_copy(w1_hbm.at[0], w1, in_sem.at[0])
    w2_copy = pltpu.make_async_copy(w2_hbm.at[0], w2, in_sem.at[1])
    centre_copy = pltpu.make_async_copy(centre_hbm, raw, in_sem.at[2])
    embed_copy = pltpu.make_async_copy(embed_hbm, embed, in_sem.at[3])

    def x_copy(m):
        return pltpu.make_async_copy(x_hbm.at[m], xin.at[m], x_sem.at[m])

    @pl.when(first)
    def _():
        for m in range(images):
            x_copy(m).start()

    @pl.when(last)
    def _():
        centre_copy.start()

    w1_copy.start()
    w2_copy.start()

    @pl.when(last)
    def _():
        embed_copy.start()

    barrier = pltpu.get_barrier_semaphore()

    @pl.when(section > 0)
    def _():
        pl.semaphore_signal(barrier, inc=1, device_id={"section": section - 1}, device_id_type=MESH)

    @pl.when(section < sections - 1)
    def _():
        pl.semaphore_signal(barrier, inc=1, device_id={"section": section + 1}, device_id_type=MESH)

    @pl.when(last)
    def _():
        @pl.loop(1, shards)
        def _(k):
            peer = lax.rem(me + k, shards)
            pl.semaphore_signal(barrier, inc=1, device_id={"shard": peer}, device_id_type=MESH)

    q = lax.broadcasted_iota(jnp.int32, (rows, positions), 0)
    p = lax.broadcasted_iota(jnp.int32, (rows, positions), 1)
    j = q & (STRIDE - 1)
    expand[...] = jnp.where((p == side * (q >> ROW_BITS) + j) & (j < side), 1.0, 0.0).astype(bf16)
    q = lax.broadcasted_iota(jnp.int32, (positions, rows), 1)
    p = lax.broadcasted_iota(jnp.int32, (positions, rows), 0)
    j = q & (STRIDE - 1)
    compact[...] = jnp.where((p == side * (q >> ROW_BITS) + j) & (j < side), 1.0, 0.0).astype(bf16)
    keep = (lax.broadcasted_iota(jnp.int32, (rows, channels), 0) & (STRIDE - 1)) < side

    for cols in (cols_a, cols_b):
        cols[pl.ds(0, STRIDE), :] = jnp.zeros((STRIDE, 3 * channels), bf16)
        cols[pl.ds(rows + STRIDE, STRIDE), :] = jnp.zeros((STRIDE, 3 * channels), bf16)

    def put_cols(cols, value):
        body = pl.ds(STRIDE, rows)
        cols[body, pl.ds(channels, channels)] = value.astype(bf16)
        cols[body, pl.ds(0, channels)] = pltpu.roll(value, 1, 0).astype(bf16)
        cols[body, pl.ds(2 * channels, channels)] = pltpu.roll(value, rows - 1, 0).astype(bf16)

    def conv(cols, weights):
        depth = 3 * channels
        total = dot(cols[pl.ds(0, rows), :], weights[pl.ds(0, depth), :])
        for d in (1, 2):
            total += dot(cols[pl.ds(STRIDE * d, rows), :], weights[pl.ds(depth * d, depth), :])
        return total

    def flip(source, target):
        for t in range(9):
            target[pl.ds(t * channels, channels), :] = source[
                pl.ds((8 - t) * channels, channels), :
            ].T

    def to_peers(kind, source, target, k):
        peer = lax.rem(me + k, shards)
        return pltpu.make_async_remote_copy(
            src_ref=source if kind == 0 else source.at[peer],
            dst_ref=target.at[me],
            send_sem=peer_send.at[kind, k],
            recv_sem=peer_recv.at[kind, k],
            device_id={"shard": peer},
            device_id_type=MESH,
        )

    def send_peers(kind, source, target):
        @pl.loop(1, shards)
        def _(k):
            to_peers(kind, source, target, k).start()

    def recv_peers(kind, source, target):
        @pl.loop(1, shards)
        def _(k):
            sender = lax.rem(me + shards - k, shards)
            pltpu.make_async_remote_copy(
                src_ref=source if kind == 0 else source.at[sender],
                dst_ref=target.at[sender],
                send_sem=peer_send.at[kind, k],
                recv_sem=peer_recv.at[kind, k],
                device_id={"shard": sender},
                device_id_type=MESH,
            ).wait_recv()

    def drain_peers(kind, source, target):
        @pl.loop(1, shards)
        def _(k):
            to_peers(kind, source, target, k).wait_send()

    def hits():
        ids = lax.broadcasted_iota(jnp.int32, (faces, class_count), 1)
        wanted = label_col[...].astype(jnp.int32) - offset_ref[0]
        return jnp.where(wanted == ids, 1.0, 0.0)

    neighbours = jnp.where(first, 0, 1) + jnp.where(last, shards - 1, 1)
    pl.semaphore_wait(barrier, neighbours)

    @pl.when(last)
    def _():
        micro = labels_ref.shape[0]
        local = images // micro
        row = lax.broadcasted_iota(jnp.int32, (faces, labels_ref.shape[1]), 0)
        lane = lax.broadcasted_iota(jnp.int32, (faces, labels_ref.shape[1]), 1)
        column = jnp.zeros((faces, labels_ref.shape[1]), f32)
        for m in range(micro):
            for f in range(local):
                values = labels_ref[pl.ds(m, 1), :].astype(f32)
                column += jnp.where(row - lane // local * images == m * local + f, 1.0, 0.0) * (
                    jnp.where(lane % local == f, 1.0, 0.0) if local > 1 else 1.0
                ) * values
        label_col[...] = jnp.sum(column, axis=1, keepdims=True)
        dw16[...] = dot(expand[...], depth_ref[...])
        pooled[...] = jnp.zeros_like(pooled)
        gpool[...] = jnp.zeros_like(gpool)
        emb[...] = jnp.zeros_like(emb)
        centre_copy.wait()
        block = LANES

        @pl.loop(0, class_count // block)
        def _(b):
            part = pl.ds(pl.multiple_of(b * block, block), block)
            values = raw[part, :].astype(f32)
            square = jnp.mean(values * values, axis=-1, keepdims=True)
            factor = lax.rsqrt(square + tiny_value) / math.sqrt(width)
            centres[part, :] = (values * factor).astype(bf16)

        flat[...] = dot(hits().astype(bf16), centres[...])
        for n in range(shards):
            chosen_src[n] = flat[pl.ds(n * images, images), :]
        chosen_rcv[me] = chosen_src[me]
        send_peers(1, chosen_src, chosen_rcv)

    gain = gain_ref[...]
    bias = bias_ref[...]
    leak = leak_ref[...]
    w1_copy.wait()
    w2_copy.wait()

    def x_send(m, step=1):
        return pltpu.make_async_remote_copy(
            src_ref=xsend.at[m],
            dst_ref=xin.at[m],
            send_sem=xs_send.at[m],
            recv_sem=xs_recv.at[m],
            device_id={"section": section + step},
            device_id_type=MESH,
        )

    def g_send(m, step=-1):
        return pltpu.make_async_remote_copy(
            src_ref=gout.at[m],
            dst_ref=gin.at[m],
            send_sem=gs_send.at[m],
            recv_sem=gs_recv.at[m],
            device_id={"section": section + step},
            device_id_type=MESH,
        )

    @pl.loop(0, images)
    def _(m):
        @pl.when(first)
        def _():
            x_copy(m).wait()

        @pl.when(section > 0)
        def _():
            x_send(m, -1).wait_recv()

        x16 = dot(expand[...], xin[m])
        put_cols(cols_a, x16)
        z = conv(cols_a, w1) * gain + bias
        small = jnp.exp(-jnp.abs(4.0 * z))
        active = leak * z + (1.0 - leak) * (jnp.maximum(4.0 * z, 0.0) + jnp.log1p(small)) / 4.0
        put_cols(cols_b, jnp.where(keep, active, 0.0))
        share = jnp.where(z >= 0.0, 1.0, small) / (1.0 + small)
        slope[m] = jnp.where(keep, (leak + (1.0 - leak) * share) * gain, 0.0)
        y = (x16 + conv(cols_b, w2)).astype(bf16)

        @pl.when(section < sections - 1)
        def _():
            xsend[m] = dot(compact[...], y).astype(bf16)
            x_send(m).start()

        @pl.when(last)
        def _():
            pooled[pl.ds(m, 1), :] = jnp.sum(y.astype(f32) * dw16[...], axis=0, keepdims=True)

    @pl.when(section < sections - 1)
    def _():
        flip(w2, w2t)
        flip(w1, w1t)

    @pl.when(last)
    def _():
        embed_copy.wait()
        embedded = dot(pooled[...].astype(bf16), embed[...])
        square = jnp.mean(embedded * embedded, axis=-1, keepdims=True)
        factor = lax.rsqrt(square + tiny_value) / math.sqrt(width)
        normed = (embedded * factor).astype(bf16).astype(f32)
        unit_src[...] = normed[:images]
        unit_all[me] = normed[:images]
        send_peers(0, unit_src, unit_all)
        flip(w2, w2t)
        recv_peers(0, unit_src, unit_all)
        for n in range(shards):
            flat[pl.ds(n * images, images), :] = unit_all[n]
        cosines = dot_nt(flat[...].astype(bf16), centres[...])
        logits = scale_value * (cosines - margin_value * hits())
        grown = jnp.exp(logits)
        wide[:, pl.ds(0, width)] = dot(grown.astype(bf16), centres[...])
        wide[:, pl.ds(width, LANES)] = jnp.broadcast_to(
            jnp.sum(grown, axis=1, keepdims=True), (faces, LANES)
        )
        for n in range(shards):
            part_src[n] = wide[pl.ds(n * images, images), :]
        part_rcv[me] = part_src[me]
        send_peers(2, part_src, part_rcv)
        flip(w1, w1t)
        recv_peers(1, chosen_src, chosen_rcv)
        chosen = jnp.sum(chosen_rcv[...], axis=0)
        recv_peers(2, part_src, part_rcv)
        sums = jnp.sum(part_rcv[...], axis=0)
        grad_unit = scale_value * (sums[:, :width] / sums[:, width : width + 1] - chosen)
        embedded = embedded[:images]
        inner = jnp.sum(embedded * grad_unit, axis=-1, keepdims=True)
        grad_embed = factor[:images] * (
            grad_unit - embedded * inner / (width * (square[:images] + tiny_value))
        )
        emb[pl.ds(0, images), :] = grad_embed
        gpool[...] = dot_nt(emb[...].astype(bf16), embed[...])

    def out_copy(m):
        return pltpu.make_async_copy(gout.at[m], out_hbm.at[m], out_sem.at[m])

    @pl.loop(0, images)
    def _(m):
        @pl.when(last)
        def _():
            g16[...] = (gpool[pl.ds(m, 1), :] * dw16[...]).astype(bf16).astype(f32)

        @pl.when(section < sections - 1)
        def _():
            g_send(m, 1).wait_recv()
            g16[...] = dot(expand[...], gin[m])

        put_cols(cols_a, g16[...])
        grad_hidden = conv(cols_a, w2t) * slope[m]
        put_cols(cols_b, grad_hidden)
        result = (g16[...] + conv(cols_b, w1t)).astype(bf16)
        gout[m] = dot(compact[...], result).astype(bf16)

        @pl.when(section > 0)
        def _():
            g_send(m).start()

        out_copy(m).start()

    @pl.loop(0, images)
    def _(m):
        @pl.when(section < sections - 1)
        def _():
            x_send(m).wait_send()

        @pl.when(section > 0)
        def _():
            g_send(m).wait_send()

        out_copy(m).wait()

    @pl.when(last)
    def _():
        drain_peers(0, unit_src, unit_all)
        drain_peers(1, chosen_src, chosen_rcv)
        drain_peers(2, part_src, part_rcv)


def on_device(
    section_input,
    conv_one,
    conv_two,
    unit_gain,
    offset_bias,
    leak_slope,
    depthwise,
    embed_weight,
    class_centers,
    labels,
    class_offsets,
):
    sections = lax.axis_size("section")
    shards = lax.axis_size("shard")
    micro, local, positions, channels = section_input.shape
    side = math.isqrt(positions)
    images = micro * local
    rows = side * STRIDE
    width = embed_weight.shape[1]
    classes = class_centers.shape[0]
    faces = shards * images
    face_rows = -(-images // HALF_ROWS) * HALF_ROWS
    vmem = pl.BlockSpec(memory_space=pltpu.VMEM)
    smem = pl.BlockSpec(memory_space=pltpu.SMEM)
    hbm = pl.BlockSpec(memory_space=pl.ANY)
    dma = pltpu.SemaphoreType.DMA
    maps = pltpu.VMEM((images, positions, channels), bf16)
    weights = pltpu.VMEM(conv_one.shape[1:], bf16)
    columns = pltpu.VMEM((rows + 2 * STRIDE, 3 * channels), bf16)
    result = pl.pallas_call(
        functools.partial(kernel, sections, shards, images, side),
        out_shape=jax.ShapeDtypeStruct((images, positions, channels), bf16),
        in_specs=[hbm, hbm, hbm, vmem, vmem, vmem, vmem, hbm, hbm, vmem, smem],
        out_specs=hbm,
        scratch_shapes=[
            maps,
            maps,
            maps,
            maps,
            weights,
            weights,
            weights,
            weights,
            pltpu.VMEM(embed_weight.shape, bf16),
            pltpu.VMEM((classes, width), bf16),
            pltpu.VMEM((classes, width), bf16),
            columns,
            columns,
            pltpu.VMEM((rows, positions), bf16),
            pltpu.VMEM((positions, rows), bf16),
            pltpu.VMEM((rows, channels), f32),
            pltpu.VMEM((images, rows, channels), f32),
            pltpu.VMEM((rows, channels), f32),
            pltpu.VMEM((face_rows, channels), f32),
            pltpu.VMEM((face_rows, width), f32),
            pltpu.VMEM((face_rows, channels), f32),
            pltpu.VMEM((images, width), f32),
            pltpu.VMEM((shards, images, width), f32),
            pltpu.VMEM((faces, width), f32),
            pltpu.VMEM((faces, width + LANES), f32),
            pltpu.VMEM((faces, 1), f32),
            pltpu.VMEM((shards, images, width), f32),
            pltpu.VMEM((shards, images, width), f32),
            pltpu.VMEM((shards, images, width + LANES), f32),
            pltpu.VMEM((shards, images, width + LANES), f32),
            dma((4,)),
            dma((images,)),
            dma((images,)),
            dma((images,)),
            dma((images,)),
            dma((images,)),
            dma((images,)),
            dma((3, shards)),
            dma((3, shards)),
        ],
        compiler_params=pltpu.CompilerParams(
            collective_id=0, has_side_effects=True, vmem_limit_bytes=60000 * 1024
        ),
        name="window",
    )(
        section_input.reshape(images, positions, channels),
        conv_one,
        conv_two,
        unit_gain,
        offset_bias,
        leak_slope,
        depthwise,
        embed_weight,
        class_centers,
        labels,
        class_offsets,
    )
    return result.reshape(1, micro, local, positions, channels)


def solution(mesh):
    placed = (
        P(None, "shard", None, None),
        P("section", None, None),
        P("section", None, None),
        P("section", None),
        P("section", None),
        P("section", None),
        P(),
        P(),
        P("shard", None),
        P(),
        P("shard"),
    )
    return jax.shard_map(
        on_device,
        mesh=mesh,
        in_specs=placed,
        out_specs=P("section", None, "shard", None, None),
        check_vma=False,
    )
```

```python
import functools
import math

import jax
import jax.numpy as jnp
from jax import lax
from jax.experimental import pallas as pl
from jax.experimental.pallas import tpu as pltpu
from jax.sharding import PartitionSpec as P

MESH = pl.DeviceIdType.MESH
STRIDE = 16
ROW_BITS = 4
HALF_ROWS = 16
LANES = 128

margin_value = 0.4
scale_value = 64.0
tiny_value = 1e-06

f32 = jnp.float32
bf16 = jnp.bfloat16


def dot(left, right):
    return jnp.dot(left, right, preferred_element_type=f32)


def dot_nt(left, right):
    return lax.dot_general(left, right, (((1,), (1,)), ((), ())), preferred_element_type=f32)


def kernel(
    sections,
    shards,
    images,
    side,
    x_hbm,
    w1_hbm,
    w2_hbm,
    gain_ref,
    bias_ref,
    leak_ref,
    depth_ref,
    embed_hbm,
    centre_hbm,
    labels_ref,
    offset_ref,
    out_hbm,
    xin,
    xsend,
    gin,
    gout,
    w1,
    w2,
    w1t,
    w2t,
    embed,
    raw,
    centres,
    cols_a,
    cols_b,
    expand,
    compact,
    dw16,
    slope,
    g16,
    pooled,
    emb,
    gemb,
    unit_src,
    unit_all,
    flat,
    wide,
    label_col,
    hits,
    picked,
    chosen_src,
    chosen_rcv,
    part_src,
    part_rcv,
    in_sem,
    x_sem,
    xs_send,
    xs_recv,
    gs_send,
    gs_recv,
    out_sem,
    peer_send,
    peer_recv,
):
    section = lax.axis_index("section")
    me = lax.axis_index("shard")
    first = section == 0
    last = section == sections - 1
    positions = side * side
    rows = side * STRIDE
    channels = w1.shape[1]
    width = embed.shape[1]
    class_count = centres.shape[0]

    w1_copy = pltpu.make_async_copy(w1_hbm.at[0], w1, in_sem.at[0])
    w2_copy = pltpu.make_async_copy(w2_hbm.at[0], w2, in_sem.at[1])
    centre_copy = pltpu.make_async_copy(centre_hbm, raw, in_sem.at[2])
    embed_copy = pltpu.make_async_copy(embed_hbm, embed, in_sem.at[3])

    def x_copy(m):
        return pltpu.make_async_copy(x_hbm.at[m], xin.at[m], x_sem.at[m])

    @pl.when(first)
    def _():
        for m in range(images):
            x_copy(m).start()

    @pl.when(last)
    def _():
        centre_copy.start()

    w1_copy.start()
    w2_copy.start()

    @pl.when(last)
    def _():
        embed_copy.start()

    barrier = pltpu.get_barrier_semaphore()

    @pl.when(section > 0)
    def _():
        pl.semaphore_signal(barrier, inc=1, device_id={"section": section - 1}, device_id_type=MESH)

    @pl.when(section < sections - 1)
    def _():
        pl.semaphore_signal(barrier, inc=1, device_id={"section": section + 1}, device_id_type=MESH)

    @pl.when(last)
    def _():
        @pl.loop(1, shards)
        def _(k):
            peer = lax.rem(me + k, shards)
            pl.semaphore_signal(barrier, inc=1, device_id={"shard": peer}, device_id_type=MESH)

    q = lax.broadcasted_iota(jnp.int32, (rows, positions), 0)
    p = lax.broadcasted_iota(jnp.int32, (rows, positions), 1)
    j = q & (STRIDE - 1)
    expand[...] = jnp.where((p == side * (q >> ROW_BITS) + j) & (j < side), 1.0, 0.0).astype(bf16)
    q = lax.broadcasted_iota(jnp.int32, (positions, rows), 1)
    p = lax.broadcasted_iota(jnp.int32, (positions, rows), 0)
    j = q & (STRIDE - 1)
    compact[...] = jnp.where((p == side * (q >> ROW_BITS) + j) & (j < side), 1.0, 0.0).astype(bf16)
    keep = (lax.broadcasted_iota(jnp.int32, (rows, channels), 0) & (STRIDE - 1)) < side

    for cols in (cols_a, cols_b):
        cols[pl.ds(0, STRIDE), :] = jnp.zeros((STRIDE, 3 * channels), bf16)
        cols[pl.ds(rows + STRIDE, STRIDE), :] = jnp.zeros((STRIDE, 3 * channels), bf16)

    def put_cols(cols, value):
        body = pl.ds(STRIDE, rows)
        cols[body, pl.ds(channels, channels)] = value.astype(bf16)
        cols[body, pl.ds(0, channels)] = pltpu.roll(value, 1, 0).astype(bf16)
        cols[body, pl.ds(2 * channels, channels)] = pltpu.roll(value, rows - 1, 0).astype(bf16)

    def conv(cols, weights):
        depth = 3 * channels
        total = dot(cols[pl.ds(0, rows), :], weights[pl.ds(0, depth), :])
        for d in (1, 2):
            total += dot(cols[pl.ds(STRIDE * d, rows), :], weights[pl.ds(depth * d, depth), :])
        return total

    def flip(source, target):
        for t in range(9):
            target[pl.ds(t * channels, channels), :] = source[
                pl.ds((8 - t) * channels, channels), :
            ].T

    sources = (unit_src, chosen_src, part_src)
    targets = (unit_all, chosen_rcv, part_rcv)

    def peer_copy(kind, m, k, to, slot):
        source = sources[kind].at[m]
        return pltpu.make_async_remote_copy(
            src_ref=source if kind == 0 else source.at[to],
            dst_ref=targets[kind].at[m, slot],
            send_sem=peer_send.at[kind, m, k],
            recv_sem=peer_recv.at[kind, m, k],
            device_id={"shard": to},
            device_id_type=MESH,
        )

    def send_peers(kind, m):
        @pl.loop(1, shards)
        def _(k):
            peer_copy(kind, m, k, lax.rem(me + k, shards), me).start()

    def recv_peers(kind, m):
        @pl.loop(1, shards)
        def _(k):
            sender = lax.rem(me + shards - k, shards)
            peer_copy(kind, m, k, sender, sender).wait_recv()

    def drain_peers(kind, m):
        @pl.loop(1, shards)
        def _(k):
            peer_copy(kind, m, k, lax.rem(me + k, shards), me).wait_send()

    neighbours = jnp.where(first, 0, 1) + jnp.where(last, shards - 1, 1)
    pl.semaphore_wait(barrier, neighbours)

    @pl.when(last)
    def _():
        micro = labels_ref.shape[0]
        local = images // micro
        row = lax.broadcasted_iota(jnp.int32, (shards, labels_ref.shape[1]), 0)
        lane = lax.broadcasted_iota(jnp.int32, (shards, labels_ref.shape[1]), 1)
        for m in range(micro):
            values = labels_ref[pl.ds(m, 1), :].astype(f32)
            for f in range(local):
                mine = jnp.where(lane == row * local + f, values, 0.0)
                label_col[m * local + f] = jnp.sum(mine, axis=1, keepdims=True)
        dw16[...] = dot(expand[...], depth_ref[...])
        pooled[...] = jnp.zeros_like(pooled)
        gemb[...] = jnp.zeros_like(gemb)
        centre_copy.wait()
        block = LANES

        @pl.loop(0, class_count // block)
        def _(b):
            part = pl.ds(pl.multiple_of(b * block, block), block)
            values = raw[part, :].astype(f32)
            square = jnp.mean(values * values, axis=-1, keepdims=True)
            factor = lax.rsqrt(square + tiny_value) / math.sqrt(width)
            centres[part, :] = (values * factor).astype(bf16)

        ids = lax.broadcasted_iota(jnp.int32, (shards, class_count), 1)

        for m in range(images):
            wanted = label_col[m].astype(jnp.int32) - offset_ref[0]
            hit = jnp.where(wanted == ids, 1.0, 0.0).astype(bf16)
            hits[pl.ds(m * shards, shards), :] = hit
        picked[...] = dot(hits[...], centres[...])
        for m in range(images):
            for n in range(shards):
                chosen_src[m, n] = picked[pl.ds(m * shards + n, 1), :]
            chosen_rcv[m, me] = chosen_src[m, me]
            send_peers(1, m)

        w1_copy.wait()
        w2_copy.wait()
        flip(w2, w2t)
        flip(w1, w1t)

    gain = gain_ref[...]
    bias = bias_ref[...]
    leak = leak_ref[...]

    @pl.when(section < sections - 1)
    def _():
        w1_copy.wait()
        w2_copy.wait()

    def x_send(m, step=1):
        return pltpu.make_async_remote_copy(
            src_ref=xsend.at[m],
            dst_ref=xin.at[m],
            send_sem=xs_send.at[m],
            recv_sem=xs_recv.at[m],
            device_id={"section": section + step},
            device_id_type=MESH,
        )

    def g_send(m, step=-1):
        return pltpu.make_async_remote_copy(
            src_ref=gout.at[m],
            dst_ref=gin.at[m],
            send_sem=gs_send.at[m],
            recv_sem=gs_recv.at[m],
            device_id={"section": section + step},
            device_id_type=MESH,
        )

    def out_copy(m):
        return pltpu.make_async_copy(gout.at[m], out_hbm.at[m], out_sem.at[m])

    def forward(m):
        @pl.when(first)
        def _():
            x_copy(m).wait()

        @pl.when(section > 0)
        def _():
            x_send(m, -1).wait_recv()

        x16 = dot(expand[...], xin[m])
        put_cols(cols_a, x16)
        z = conv(cols_a, w1) * gain + bias
        small = jnp.exp(-jnp.abs(4.0 * z))
        active = leak * z + (1.0 - leak) * (jnp.maximum(4.0 * z, 0.0) + jnp.log1p(small)) / 4.0
        put_cols(cols_b, jnp.where(keep, active, 0.0))
        share = jnp.where(z >= 0.0, 1.0, small) / (1.0 + small)
        slope[m] = jnp.where(keep, (leak + (1.0 - leak) * share) * gain, 0.0)
        y = (x16 + conv(cols_b, w2)).astype(bf16)

        @pl.when(section < sections - 1)
        def _():
            xsend[m] = dot(compact[...], y).astype(bf16)
            x_send(m).start()

        @pl.when(last)
        def _():
            pooled[pl.ds(0, 1), :] = jnp.sum(y.astype(f32) * dw16[...], axis=0, keepdims=True)

            @pl.when(m == 0)
            def _():
                embed_copy.wait()

            embedded = dot(pooled[...].astype(bf16), embed[...])[:1]
            square = jnp.mean(embedded * embedded, axis=-1, keepdims=True)
            factor = lax.rsqrt(square + tiny_value) / math.sqrt(width)
            normed = (embedded * factor).astype(bf16).astype(f32)
            emb[m] = embedded
            unit_src[m] = normed
            unit_all[m, me] = normed
            send_peers(0, m)

    def partial(m):
        recv_peers(0, m)
        for n in range(shards):
            flat[pl.ds(n, 1), :] = unit_all[m, n]
        cosines = dot_nt(flat[...].astype(bf16), centres[...])
        ids = lax.broadcasted_iota(jnp.int32, (shards, class_count), 1)
        wanted = label_col[m].astype(jnp.int32) - offset_ref[0]
        logits = scale_value * (cosines - margin_value * jnp.where(wanted == ids, 1.0, 0.0))
        grown = jnp.exp(logits)
        wide[:, pl.ds(0, width)] = dot(grown.astype(bf16), centres[...])
        wide[:, pl.ds(width, LANES)] = jnp.broadcast_to(
            jnp.sum(grown, axis=1, keepdims=True), (shards, LANES)
        )
        for n in range(shards):
            part_src[m, n] = wide[pl.ds(n, 1), :]
        part_rcv[m, me] = part_src[m, me]
        send_peers(2, m)

    def backward(m):
        @pl.when(last)
        def _():
            recv_peers(1, m)
            chosen = jnp.sum(chosen_rcv[m], axis=0)
            recv_peers(2, m)
            sums = jnp.sum(part_rcv[m], axis=0)
            grad_unit = scale_value * (sums[:, :width] / sums[:, width : width + 1] - chosen)
            embedded = emb[m]
            square = jnp.mean(embedded * embedded, axis=-1, keepdims=True)
            factor = lax.rsqrt(square + tiny_value) / math.sqrt(width)
            inner = jnp.sum(embedded * grad_unit, axis=-1, keepdims=True)
            grad_embed = factor * (
                grad_unit - embedded * inner / (width * (square + tiny_value))
            )
            gemb[pl.ds(0, 1), :] = grad_embed
            gpool = dot_nt(gemb[...].astype(bf16), embed[...])[:1]
            g16[...] = (gpool * dw16[...]).astype(bf16).astype(f32)

        @pl.when(section < sections - 1)
        def _():
            g_send(m, 1).wait_recv()
            g16[...] = dot(expand[...], gin[m])

        put_cols(cols_a, g16[...])
        grad_hidden = conv(cols_a, w2t) * slope[m]
        put_cols(cols_b, grad_hidden)
        result = (g16[...] + conv(cols_b, w1t)).astype(bf16)
        gout[m] = dot(compact[...], result).astype(bf16)

        @pl.when(section > 0)
        def _():
            g_send(m).start()

        out_copy(m).start()

    @pl.loop(0, images + 3)
    def _(t):
        @pl.when(t < images)
        def _():
            forward(t)

        @pl.when((section < sections - 1) & (t == images - 1))
        def _():
            flip(w2, w2t)
            flip(w1, w1t)

        @pl.when(last & (t >= 1) & (t < images + 1))
        def _():
            partial(t - 1)

        @pl.when(t >= 3)
        def _():
            backward(t - 3)

    @pl.loop(0, images)
    def _(m):
        @pl.when(section < sections - 1)
        def _():
            x_send(m).wait_send()

        @pl.when(section > 0)
        def _():
            g_send(m).wait_send()

        out_copy(m).wait()

    @pl.when(last)
    def _():
        @pl.loop(0, images)
        def _(m):
            for kind in range(3):
                drain_peers(kind, m)


def on_device(
    section_input,
    conv_one,
    conv_two,
    unit_gain,
    offset_bias,
    leak_slope,
    depthwise,
    embed_weight,
    class_centers,
    labels,
    class_offsets,
):
    sections = lax.axis_size("section")
    shards = lax.axis_size("shard")
    micro, local, positions, channels = section_input.shape
    side = math.isqrt(positions)
    images = micro * local
    rows = side * STRIDE
    width = embed_weight.shape[1]
    classes = class_centers.shape[0]
    faces = shards * images
    vmem = pl.BlockSpec(memory_space=pltpu.VMEM)
    smem = pl.BlockSpec(memory_space=pltpu.SMEM)
    hbm = pl.BlockSpec(memory_space=pl.ANY)
    dma = pltpu.SemaphoreType.DMA
    maps = pltpu.VMEM((images, positions, channels), bf16)
    weights = pltpu.VMEM(conv_one.shape[1:], bf16)
    columns = pltpu.VMEM((rows + 2 * STRIDE, 3 * channels), bf16)
    result = pl.pallas_call(
        functools.partial(kernel, sections, shards, images, side),
        out_shape=jax.ShapeDtypeStruct((images, positions, channels), bf16),
        in_specs=[hbm, hbm, hbm, vmem, vmem, vmem, vmem, hbm, hbm, vmem, smem],
        out_specs=hbm,
        scratch_shapes=[
            maps,
            maps,
            maps,
            maps,
            weights,
            weights,
            weights,
            weights,
            pltpu.VMEM(embed_weight.shape, bf16),
            pltpu.VMEM((classes, width), bf16),
            pltpu.VMEM((classes, width), bf16),
            columns,
            columns,
            pltpu.VMEM((rows, positions), bf16),
            pltpu.VMEM((positions, rows), bf16),
            pltpu.VMEM((rows, channels), f32),
            pltpu.VMEM((images, rows, channels), f32),
            pltpu.VMEM((rows, channels), f32),
            pltpu.VMEM((HALF_ROWS, channels), f32),
            pltpu.VMEM((images, 1, width), f32),
            pltpu.VMEM((HALF_ROWS, width), f32),
            pltpu.VMEM((images, 1, width), f32),
            pltpu.VMEM((images, shards, 1, width), f32),
            pltpu.VMEM((shards, width), f32),
            pltpu.VMEM((shards, width + LANES), f32),
            pltpu.VMEM((images, shards, 1), f32),
            pltpu.VMEM((faces, classes), bf16),
            pltpu.VMEM((faces, width), f32),
            pltpu.VMEM((images, shards, 1, width), f32),
            pltpu.VMEM((images, shards, 1, width), f32),
            pltpu.VMEM((images, shards, 1, width + LANES), f32),
            pltpu.VMEM((images, shards, 1, width + LANES), f32),
            dma((4,)),
            dma((images,)),
            dma((images,)),
            dma((images,)),
            dma((images,)),
            dma((images,)),
            dma((images,)),
            dma((3, images, shards)),
            dma((3, images, shards)),
        ],
        compiler_params=pltpu.CompilerParams(
            collective_id=0, has_side_effects=True, vmem_limit_bytes=60000 * 1024
        ),
        name="window",
    )(
        section_input.reshape(images, positions, channels),
        conv_one,
        conv_two,
        unit_gain,
        offset_bias,
        leak_slope,
        depthwise,
        embed_weight,
        class_centers,
        labels,
        class_offsets,
    )
    return result.reshape(1, micro, local, positions, channels)


def solution(mesh):
    placed = (
        P(None, "shard", None, None),
        P("section", None, None),
        P("section", None, None),
        P("section", None),
        P("section", None),
        P("section", None),
        P(),
        P(),
        P("shard", None),
        P(),
        P("shard"),
    )
    return jax.shard_map(
        on_device,
        mesh=mesh,
        in_specs=placed,
        out_specs=P("section", None, "shard", None, None),
        check_vma=False,
    )
```

```python
import functools
import math

import jax
import jax.numpy as jnp
from jax import lax
from jax.experimental import pallas as pl
from jax.experimental.pallas import tpu as pltpu
from jax.sharding import PartitionSpec as P

MESH = pl.DeviceIdType.MESH
STRIDE = 16
ROW_BITS = 4
HALF_ROWS = 16
LANES = 128

margin_value = 0.4
scale_value = 64.0
tiny_value = 1e-06

f32 = jnp.float32
bf16 = jnp.bfloat16


def dot(left, right):
    return jnp.dot(left, right, preferred_element_type=f32)


def dot_nt(left, right):
    return lax.dot_general(left, right, (((1,), (1,)), ((), ())), preferred_element_type=f32)


def kernel(
    sections,
    shards,
    images,
    side,
    x_hbm,
    w1_hbm,
    w2_hbm,
    gain_ref,
    bias_ref,
    leak_ref,
    depth_ref,
    embed_hbm,
    centre_hbm,
    labels_ref,
    offset_ref,
    out_hbm,
    xin,
    xsend,
    gin,
    gout,
    w1,
    w2,
    w1t,
    w2t,
    embed,
    raw,
    centres,
    cols_a,
    cols_b,
    expand,
    compact,
    dw16,
    slope,
    g16,
    pooled,
    emb,
    gemb,
    unit_src,
    unit_all,
    flat,
    wide,
    label_col,
    hits,
    picked,
    chosen_src,
    chosen_rcv,
    part_src,
    part_rcv,
    in_sem,
    x_sem,
    xs_send,
    xs_recv,
    gs_send,
    gs_recv,
    out_sem,
    peer_send,
    peer_recv,
):
    section = lax.axis_index("section")
    me = lax.axis_index("shard")
    first = section == 0
    last = section == sections - 1
    positions = side * side
    rows = side * STRIDE
    channels = w1.shape[1]
    width = embed.shape[1]
    class_count = centres.shape[0]
    faces = images * shards

    w1_copy = pltpu.make_async_copy(w1_hbm.at[0], w1, in_sem.at[0])
    w2_copy = pltpu.make_async_copy(w2_hbm.at[0], w2, in_sem.at[1])
    centre_copy = pltpu.make_async_copy(centre_hbm, raw, in_sem.at[2])
    embed_copy = pltpu.make_async_copy(embed_hbm, embed, in_sem.at[3])

    def x_copy(m):
        return pltpu.make_async_copy(x_hbm.at[m], xin.at[m], x_sem.at[m])

    @pl.when(first)
    def _():
        for m in range(images):
            x_copy(m).start()

    @pl.when(last)
    def _():
        centre_copy.start()

    w1_copy.start()
    w2_copy.start()

    @pl.when(last)
    def _():
        embed_copy.start()

    barrier = pltpu.get_barrier_semaphore()

    @pl.when(section > 0)
    def _():
        pl.semaphore_signal(barrier, inc=1, device_id={"section": section - 1}, device_id_type=MESH)

    @pl.when(section < sections - 1)
    def _():
        pl.semaphore_signal(barrier, inc=1, device_id={"section": section + 1}, device_id_type=MESH)

    @pl.when(last)
    def _():
        @pl.loop(1, shards)
        def _(k):
            peer = lax.rem(me + k, shards)
            pl.semaphore_signal(barrier, inc=1, device_id={"shard": peer}, device_id_type=MESH)

    q = lax.broadcasted_iota(jnp.int32, (rows, positions), 0)
    p = lax.broadcasted_iota(jnp.int32, (rows, positions), 1)
    j = q & (STRIDE - 1)
    expand[...] = jnp.where((p == side * (q >> ROW_BITS) + j) & (j < side), 1.0, 0.0).astype(bf16)
    q = lax.broadcasted_iota(jnp.int32, (positions, rows), 1)
    p = lax.broadcasted_iota(jnp.int32, (positions, rows), 0)
    j = q & (STRIDE - 1)
    compact[...] = jnp.where((p == side * (q >> ROW_BITS) + j) & (j < side), 1.0, 0.0).astype(bf16)
    keep = (lax.broadcasted_iota(jnp.int32, (rows, channels), 0) & (STRIDE - 1)) < side

    for cols in (cols_a, cols_b):
        cols[pl.ds(0, STRIDE), :] = jnp.zeros((STRIDE, 3 * channels), bf16)
        cols[pl.ds(rows + STRIDE, STRIDE), :] = jnp.zeros((STRIDE, 3 * channels), bf16)

    def put_cols(cols, value):
        body = pl.ds(STRIDE, rows)
        cols[body, pl.ds(channels, channels)] = value.astype(bf16)
        cols[body, pl.ds(0, channels)] = pltpu.roll(value, 1, 0).astype(bf16)
        cols[body, pl.ds(2 * channels, channels)] = pltpu.roll(value, rows - 1, 0).astype(bf16)

    def conv(cols, weights):
        depth = 3 * channels
        total = dot(cols[pl.ds(0, rows), :], weights[pl.ds(0, depth), :])
        for d in (1, 2):
            total += dot(cols[pl.ds(STRIDE * d, rows), :], weights[pl.ds(depth * d, depth), :])
        return total

    def flip(source, target):
        for t in range(9):
            target[pl.ds(t * channels, channels), :] = source[
                pl.ds((8 - t) * channels, channels), :
            ].T

    sources = (unit_src, chosen_src, part_src)
    targets = (unit_all, chosen_rcv, part_rcv)

    def peer_copy(kind, m, to):
        source = sources[kind].at[m]
        return pltpu.make_async_remote_copy(
            src_ref=source if kind == 0 else source.at[to],
            dst_ref=targets[kind].at[m, me],
            send_sem=peer_send.at[kind, m],
            recv_sem=peer_recv.at[kind, m],
            device_id={"shard": to},
            device_id_type=MESH,
        )

    def send_peers(kind, m):
        @pl.loop(1, shards)
        def _(k):
            peer_copy(kind, m, lax.rem(me + k, shards)).start()

    def peers_all(kind, m):
        others = targets[kind].at[m, pl.ds(0, shards - 1)]
        return pltpu.make_async_remote_copy(
            src_ref=others,
            dst_ref=others,
            send_sem=peer_send.at[kind, m],
            recv_sem=peer_recv.at[kind, m],
            device_id={"shard": lax.rem(me + 1, shards)},
            device_id_type=MESH,
        )

    def recv_peers(kind, m):
        peers_all(kind, m).wait_recv()

    def drain_peers(kind, m):
        peers_all(kind, m).wait_send()

    @pl.when(last)
    def _():
        micro = labels_ref.shape[0]
        local = images // micro
        row = lax.broadcasted_iota(jnp.int32, (shards, labels_ref.shape[1]), 0)
        lane = lax.broadcasted_iota(jnp.int32, (shards, labels_ref.shape[1]), 1)
        for m in range(micro):
            values = labels_ref[pl.ds(m, 1), :].astype(f32)
            for f in range(local):
                mine = jnp.where(lane == row * local + f, values, 0.0)
                label_col[pl.ds((m * local + f) * shards, shards), :] = jnp.sum(mine, axis=1, keepdims=True)
        dw16[...] = dot(expand[...], depth_ref[...])
        pooled[...] = jnp.zeros_like(pooled)
        gemb[...] = jnp.zeros_like(gemb)
        with jax.named_scope("centre_wait"):
            centre_copy.wait()
        block = LANES

        @pl.loop(0, class_count // block)
        def _(b):
            part = pl.ds(pl.multiple_of(b * block, block), block)
            values = raw[part, :].astype(f32)
            square = jnp.mean(values * values, axis=-1, keepdims=True)
            factor = lax.rsqrt(square + tiny_value) / math.sqrt(width)
            centres[part, :] = (values * factor).astype(bf16)

        ids = lax.broadcasted_iota(jnp.int32, (faces, class_count), 1)
        wanted = label_col[...].astype(jnp.int32) - offset_ref[0]
        hits[...] = jnp.where(wanted == ids, 1.0, 0.0).astype(bf16)
        picked[...] = dot(hits[...], centres[...])
        for m in range(images):
            for n in range(shards):
                chosen_src[m, n] = picked[pl.ds(m * shards + n, 1), :]
            chosen_rcv[m, me] = chosen_src[m, me]

        with jax.named_scope("w_wait"):
            w1_copy.wait()
            w2_copy.wait()
        with jax.named_scope("flip"):
            flip(w2, w2t)
            flip(w1, w1t)

    neighbours = jnp.where(first, 0, 1) + jnp.where(last, shards - 1, 1)
    with jax.named_scope("barrier"):
        pl.semaphore_wait(barrier, neighbours)

    @pl.when(last)
    def _():
        @pl.loop(0, images)
        def _(m):
            send_peers(1, m)

    gain = gain_ref[...]
    bias = bias_ref[...]
    leak = leak_ref[...]

    @pl.when(section < sections - 1)
    def _():
        with jax.named_scope("w_wait"):
            w1_copy.wait()
            w2_copy.wait()

    def x_send(m, step=1):
        return pltpu.make_async_remote_copy(
            src_ref=xsend.at[m],
            dst_ref=xin.at[m],
            send_sem=xs_send.at[m],
            recv_sem=xs_recv.at[m],
            device_id={"section": section + step},
            device_id_type=MESH,
        )

    def g_send(m, step=-1):
        return pltpu.make_async_remote_copy(
            src_ref=gout.at[m],
            dst_ref=gin.at[m],
            send_sem=gs_send.at[m],
            recv_sem=gs_recv.at[m],
            device_id={"section": section + step},
            device_id_type=MESH,
        )

    def out_copy(m):
        return pltpu.make_async_copy(gout.at[m], out_hbm.at[m], out_sem.at[m])

    def forward(m):
        @pl.when(first)
        def _():
            x_copy(m).wait()

        @pl.when(section > 0)
        def _():
            with jax.named_scope("x_wait"):
                x_send(m, -1).wait_recv()

        x16 = dot(expand[...], xin[m])
        put_cols(cols_a, x16)
        z = conv(cols_a, w1) * gain + bias
        small = jnp.exp(-jnp.abs(4.0 * z))
        active = leak * z + (1.0 - leak) * (jnp.maximum(4.0 * z, 0.0) + jnp.log1p(small)) / 4.0
        put_cols(cols_b, jnp.where(keep, active, 0.0))
        share = jnp.where(z >= 0.0, 1.0, small) / (1.0 + small)
        slope[m] = jnp.where(keep, (leak + (1.0 - leak) * share) * gain, 0.0)
        y = (x16 + conv(cols_b, w2)).astype(bf16)

        @pl.when(section < sections - 1)
        def _():
            xsend[m] = dot(compact[...], y).astype(bf16)
            x_send(m).start()

        @pl.when(last)
        def _():
            pooled[pl.ds(0, 1), :] = jnp.sum(y.astype(f32) * dw16[...], axis=0, keepdims=True)

            @pl.when(m == 0)
            def _():
                embed_copy.wait()

            embedded = dot(pooled[...].astype(bf16), embed[...])[:1]
            square = jnp.mean(embedded * embedded, axis=-1, keepdims=True)
            factor = lax.rsqrt(square + tiny_value) / math.sqrt(width)
            normed = (embedded * factor).astype(bf16).astype(f32)
            emb[m] = embedded
            unit_src[m] = normed
            unit_all[m, me] = normed
            send_peers(0, m)

    def partial(m):
        with jax.named_scope("unit_wait"):
            recv_peers(0, m)
        for n in range(shards):
            flat[pl.ds(n, 1), :] = unit_all[m, n]
        cosines = dot_nt(flat[...].astype(bf16), centres[...])
        mine = pl.ds(pl.multiple_of(m * shards, shards), shards)
        logits = scale_value * (cosines - margin_value * hits[mine, :].astype(f32))
        grown = jnp.exp(logits)
        wide[:, pl.ds(0, width)] = dot(grown.astype(bf16), centres[...])
        wide[:, pl.ds(width, LANES)] = jnp.broadcast_to(
            jnp.sum(grown, axis=1, keepdims=True), (shards, LANES)
        )
        for n in range(shards):
            part_src[m, n] = wide[pl.ds(n, 1), :]
        part_rcv[m, me] = part_src[m, me]
        send_peers(2, m)

    def backward(m):
        @pl.when(last)
        def _():
            with jax.named_scope("chosen_wait"):
                recv_peers(1, m)
            chosen = jnp.sum(chosen_rcv[m], axis=0)
            with jax.named_scope("part_wait"):
                recv_peers(2, m)
            sums = jnp.sum(part_rcv[m], axis=0)
            grad_unit = scale_value * (sums[:, :width] / sums[:, width : width + 1] - chosen)
            embedded = emb[m]
            square = jnp.mean(embedded * embedded, axis=-1, keepdims=True)
            factor = lax.rsqrt(square + tiny_value) / math.sqrt(width)
            inner = jnp.sum(embedded * grad_unit, axis=-1, keepdims=True)
            grad_embed = factor * (
                grad_unit - embedded * inner / (width * (square + tiny_value))
            )
            gemb[pl.ds(0, 1), :] = grad_embed
            gpool = dot_nt(gemb[...].astype(bf16), embed[...])[:1]
            g16[...] = (gpool * dw16[...]).astype(bf16).astype(f32)

        @pl.when(section < sections - 1)
        def _():
            with jax.named_scope("g_wait"):
                g_send(m, 1).wait_recv()
            g16[...] = dot(expand[...], gin[m])

        put_cols(cols_a, g16[...])
        grad_hidden = conv(cols_a, w2t) * slope[m]
        put_cols(cols_b, grad_hidden)
        result = (g16[...] + conv(cols_b, w1t)).astype(bf16)
        gout[m] = dot(compact[...], result).astype(bf16)

        @pl.when(section > 0)
        def _():
            g_send(m).start()

        out_copy(m).start()

    def drain():
        @pl.loop(0, images)
        def _(m):
            @pl.when(section < sections - 1)
            def _():
                x_send(m).wait_send()

            @pl.when(section > 0)
            def _():
                g_send(m).wait_send()

            out_copy(m).wait()

        @pl.when(last)
        def _():
            @pl.loop(0, images)
            def _(m):
                for kind in range(3):
                    drain_peers(kind, m)

    lag = 4

    @pl.loop(0, images + lag)
    def _(t):
        @pl.when(t < images)
        def _():
            with jax.named_scope("forward"):
                forward(t)

        @pl.when((section < sections - 1) & (t == images - 1))
        def _():
            with jax.named_scope("flip"):
                flip(w2, w2t)
                flip(w1, w1t)

        @pl.when(last & (t >= 2) & (t < images + 2))
        def _():
            with jax.named_scope("partial"):
                partial(t - 2)

        @pl.when(t >= lag)
        def _():
            with jax.named_scope("backward"):
                backward(t - lag)

    with jax.named_scope("drain"):
        drain()


def on_device(
    section_input,
    conv_one,
    conv_two,
    unit_gain,
    offset_bias,
    leak_slope,
    depthwise,
    embed_weight,
    class_centers,
    labels,
    class_offsets,
):
    sections = lax.axis_size("section")
    shards = lax.axis_size("shard")
    micro, local, positions, channels = section_input.shape
    side = math.isqrt(positions)
    images = micro * local
    rows = side * STRIDE
    width = embed_weight.shape[1]
    classes = class_centers.shape[0]
    faces = shards * images
    vmem = pl.BlockSpec(memory_space=pltpu.VMEM)
    smem = pl.BlockSpec(memory_space=pltpu.SMEM)
    hbm = pl.BlockSpec(memory_space=pl.ANY)
    dma = pltpu.SemaphoreType.DMA
    maps = pltpu.VMEM((images, positions, channels), bf16)
    weights = pltpu.VMEM(conv_one.shape[1:], bf16)
    columns = pltpu.VMEM((rows + 2 * STRIDE, 3 * channels), bf16)
    result = pl.pallas_call(
        functools.partial(kernel, sections, shards, images, side),
        out_shape=jax.ShapeDtypeStruct((images, positions, channels), bf16),
        in_specs=[hbm, hbm, hbm, vmem, vmem, vmem, vmem, hbm, hbm, vmem, smem],
        out_specs=hbm,
        scratch_shapes=[
            maps,
            maps,
            maps,
            maps,
            weights,
            weights,
            weights,
            weights,
            pltpu.VMEM(embed_weight.shape, bf16),
            pltpu.VMEM((classes, width), bf16),
            pltpu.VMEM((classes, width), bf16),
            columns,
            columns,
            pltpu.VMEM((rows, positions), bf16),
            pltpu.VMEM((positions, rows), bf16),
            pltpu.VMEM((rows, channels), f32),
            pltpu.VMEM((images, rows, channels), f32),
            pltpu.VMEM((rows, channels), f32),
            pltpu.VMEM((HALF_ROWS, channels), f32),
            pltpu.VMEM((images, 1, width), f32),
            pltpu.VMEM((HALF_ROWS, width), f32),
            pltpu.VMEM((images, 1, width), f32),
            pltpu.VMEM((images, shards, 1, width), f32),
            pltpu.VMEM((shards, width), f32),
            pltpu.VMEM((shards, width + LANES), f32),
            pltpu.VMEM((faces, 1), f32),
            pltpu.VMEM((faces, classes), bf16),
            pltpu.VMEM((faces, width), f32),
            pltpu.VMEM((images, shards, 1, width), f32),
            pltpu.VMEM((images, shards, 1, width), f32),
            pltpu.VMEM((images, shards, 1, width + LANES), f32),
            pltpu.VMEM((images, shards, 1, width + LANES), f32),
            dma((4,)),
            dma((images,)),
            dma((images,)),
            dma((images,)),
            dma((images,)),
            dma((images,)),
            dma((images,)),
            dma((3, images)),
            dma((3, images)),
        ],
        compiler_params=pltpu.CompilerParams(
            collective_id=0, has_side_effects=True, vmem_limit_bytes=60000 * 1024
        ),
        name="window",
    )(
        section_input.reshape(images, positions, channels),
        conv_one,
        conv_two,
        unit_gain,
        offset_bias,
        leak_slope,
        depthwise,
        embed_weight,
        class_centers,
        labels,
        class_offsets,
    )
    return result.reshape(1, micro, local, positions, channels)


def solution(mesh):
    placed = (
        P(None, "shard", None, None),
        P("section", None, None),
        P("section", None, None),
        P("section", None),
        P("section", None),
        P("section", None),
        P(),
        P(),
        P("shard", None),
        P(),
        P("shard"),
    )
    return jax.shard_map(
        on_device,
        mesh=mesh,
        in_specs=placed,
        out_specs=P("section", None, "shard", None, None),
        check_vma=False,
    )
```

```python
import functools
import math

import jax
import jax.numpy as jnp
from jax import lax
from jax.experimental import pallas as pl
from jax.experimental.pallas import tpu as pltpu
from jax.sharding import PartitionSpec as P

MESH = pl.DeviceIdType.MESH
STRIDE = 16
ROW_BITS = 4
HALF_ROWS = 16
LANES = 128

margin_value = 0.4
scale_value = 64.0
tiny_value = 1e-06

f32 = jnp.float32
bf16 = jnp.bfloat16


def dot(left, right):
    return jnp.dot(left, right, preferred_element_type=f32)


def dot_nt(left, right):
    return lax.dot_general(left, right, (((1,), (1,)), ((), ())), preferred_element_type=f32)


def kernel(
    sections,
    shards,
    images,
    side,
    x_hbm,
    w1_hbm,
    w2_hbm,
    gain_ref,
    bias_ref,
    leak_ref,
    depth_ref,
    embed_hbm,
    centre_hbm,
    labels_ref,
    offset_ref,
    out_hbm,
    xt,
    xin,
    xsend,
    gin,
    gout,
    w1,
    w2,
    w1t,
    w2t,
    embed,
    raw,
    centres,
    cols_a,
    cols_b,
    expand,
    compact,
    dw16,
    slope,
    g16,
    pooled,
    emb,
    gemb,
    unit_src,
    unit_all,
    flat,
    wide,
    label_col,
    hits,
    picked,
    chosen_src,
    chosen_rcv,
    part_src,
    part_rcv,
    in_sem,
    x_sem,
    xs_send,
    xs_recv,
    gs_send,
    gs_recv,
    out_sem,
    peer_send,
    peer_recv,
):
    section = lax.axis_index("section")
    me = lax.axis_index("shard")
    first = section == 0
    last = section == sections - 1
    positions = side * side
    rows = side * STRIDE
    channels = w1.shape[1]
    width = embed.shape[1]
    class_count = centres.shape[0]
    faces = images * shards

    w1_copy = pltpu.make_async_copy(w1_hbm.at[0], w1, in_sem.at[0])
    w2_copy = pltpu.make_async_copy(w2_hbm.at[0], w2, in_sem.at[1])
    centre_copy = pltpu.make_async_copy(centre_hbm, raw, in_sem.at[2])
    embed_copy = pltpu.make_async_copy(embed_hbm, embed, in_sem.at[3])

    x_copy = pltpu.make_async_copy(x_hbm, xt, x_sem.at[0])

    @pl.when(first)
    def _():
        x_copy.start()

    @pl.when(last)
    def _():
        centre_copy.start()

    w1_copy.start()
    w2_copy.start()

    @pl.when(last)
    def _():
        embed_copy.start()

    barrier = pltpu.get_barrier_semaphore()

    @pl.when(section > 0)
    def _():
        pl.semaphore_signal(barrier, inc=1, device_id={"section": section - 1}, device_id_type=MESH)

    @pl.when(section < sections - 1)
    def _():
        pl.semaphore_signal(barrier, inc=1, device_id={"section": section + 1}, device_id_type=MESH)

    @pl.when(last)
    def _():
        @pl.loop(1, shards)
        def _(k):
            peer = lax.rem(me + k, shards)
            pl.semaphore_signal(barrier, inc=1, device_id={"shard": peer}, device_id_type=MESH)

    q = lax.broadcasted_iota(jnp.int32, (rows, positions), 0)
    p = lax.broadcasted_iota(jnp.int32, (rows, positions), 1)
    j = q & (STRIDE - 1)
    expand[...] = jnp.where((p == side * (q >> ROW_BITS) + j) & (j < side), 1.0, 0.0).astype(bf16)
    q = lax.broadcasted_iota(jnp.int32, (positions, rows), 1)
    p = lax.broadcasted_iota(jnp.int32, (positions, rows), 0)
    j = q & (STRIDE - 1)
    compact[...] = jnp.where((p == side * (q >> ROW_BITS) + j) & (j < side), 1.0, 0.0).astype(bf16)
    keep = (lax.broadcasted_iota(jnp.int32, (rows, channels), 0) & (STRIDE - 1)) < side

    for cols in (cols_a, cols_b):
        cols[pl.ds(0, STRIDE), :] = jnp.zeros((STRIDE, 3 * channels), bf16)
        cols[pl.ds(rows + STRIDE, STRIDE), :] = jnp.zeros((STRIDE, 3 * channels), bf16)

    def put_cols(cols, value):
        body = pl.ds(STRIDE, rows)
        cols[body, pl.ds(channels, channels)] = value.astype(bf16)
        cols[body, pl.ds(0, channels)] = pltpu.roll(value, 1, 0).astype(bf16)
        cols[body, pl.ds(2 * channels, channels)] = pltpu.roll(value, rows - 1, 0).astype(bf16)

    def conv(cols, weights):
        depth = 3 * channels
        total = dot(cols[pl.ds(0, rows), :], weights[pl.ds(0, depth), :])
        for d in (1, 2):
            total += dot(cols[pl.ds(STRIDE * d, rows), :], weights[pl.ds(depth * d, depth), :])
        return total

    def flip(source, target):
        for t in range(9):
            target[pl.ds(t * channels, channels), :] = source[
                pl.ds((8 - t) * channels, channels), :
            ].T

    sources = (unit_src, chosen_src, part_src)
    targets = (unit_all, chosen_rcv, part_rcv)

    def peer_copy(kind, m, to):
        source = sources[kind].at[m]
        return pltpu.make_async_remote_copy(
            src_ref=source if kind == 0 else source.at[to],
            dst_ref=targets[kind].at[m, me],
            send_sem=peer_send.at[kind, m],
            recv_sem=peer_recv.at[kind, m],
            device_id={"shard": to},
            device_id_type=MESH,
        )

    def send_peers(kind, m):
        @pl.loop(1, shards)
        def _(k):
            peer_copy(kind, m, lax.rem(me + k, shards)).start()

    def peers_all(kind, m):
        others = targets[kind].at[m, pl.ds(0, shards - 1)]
        return pltpu.make_async_remote_copy(
            src_ref=others,
            dst_ref=others,
            send_sem=peer_send.at[kind, m],
            recv_sem=peer_recv.at[kind, m],
            device_id={"shard": lax.rem(me + 1, shards)},
            device_id_type=MESH,
        )

    def recv_peers(kind, m):
        peers_all(kind, m).wait_recv()

    def drain_peers(kind, m):
        peers_all(kind, m).wait_send()

    @pl.when(last)
    def _():
        micro = labels_ref.shape[0]
        local = images // micro
        row = lax.broadcasted_iota(jnp.int32, (shards, labels_ref.shape[1]), 0)
        lane = lax.broadcasted_iota(jnp.int32, (shards, labels_ref.shape[1]), 1)
        for m in range(micro):
            values = labels_ref[pl.ds(m, 1), :].astype(f32)
            for f in range(local):
                mine = jnp.where(lane == row * local + f, values, 0.0)
                label_col[pl.ds((m * local + f) * shards, shards), :] = jnp.sum(mine, axis=1, keepdims=True)
        dw16[...] = dot(expand[...], depth_ref[...])
        pooled[...] = jnp.zeros_like(pooled)
        gemb[...] = jnp.zeros_like(gemb)
        with jax.named_scope("centre_wait"):
            centre_copy.wait()
        block = LANES

        @pl.loop(0, class_count // block)
        def _(b):
            part = pl.ds(pl.multiple_of(b * block, block), block)
            values = raw[part, :].astype(f32)
            square = jnp.mean(values * values, axis=-1, keepdims=True)
            factor = lax.rsqrt(square + tiny_value) / math.sqrt(width)
            centres[part, :] = (values * factor).astype(bf16)

        ids = lax.broadcasted_iota(jnp.int32, (faces, class_count), 1)
        wanted = label_col[...].astype(jnp.int32) - offset_ref[0]
        hits[...] = jnp.where(wanted == ids, 1.0, 0.0).astype(bf16)
        picked[...] = dot(hits[...], centres[...])
        for m in range(images):
            for n in range(shards):
                chosen_src[m, n] = picked[pl.ds(m * shards + n, 1), :]
            chosen_rcv[m, me] = chosen_src[m, me]

        with jax.named_scope("w_wait"):
            w1_copy.wait()
            w2_copy.wait()
        with jax.named_scope("flip"):
            flip(w2, w2t)
            flip(w1, w1t)

    neighbours = jnp.where(first, 0, 1) + jnp.where(last, shards - 1, 1)
    with jax.named_scope("barrier"):
        pl.semaphore_wait(barrier, neighbours)

    @pl.when(last)
    def _():
        @pl.loop(0, images)
        def _(m):
            send_peers(1, m)

    gain = gain_ref[...]
    bias = bias_ref[...]
    leak = leak_ref[...]

    @pl.when(section < sections - 1)
    def _():
        with jax.named_scope("w_wait"):
            w1_copy.wait()
            w2_copy.wait()

    def x_send(m, step=1):
        return pltpu.make_async_remote_copy(
            src_ref=xsend.at[m],
            dst_ref=xin.at[m],
            send_sem=xs_send.at[m],
            recv_sem=xs_recv.at[m],
            device_id={"section": section + step},
            device_id_type=MESH,
        )

    def g_send(m, step=-1):
        return pltpu.make_async_remote_copy(
            src_ref=gout.at[m],
            dst_ref=gin.at[m],
            send_sem=gs_send.at[m],
            recv_sem=gs_recv.at[m],
            device_id={"section": section + step},
            device_id_type=MESH,
        )

    def out_copy(m):
        return pltpu.make_async_copy(gout.at[m], out_hbm.at[m], out_sem.at[m])

    def forward(m):
        for i in range(images):

            @pl.when(first & (m == i))
            def _():
                if i == 0:
                    x_copy.wait()
                xin[i] = xt[:, i, :].astype(f32).astype(bf16)

        @pl.when(section > 0)
        def _():
            with jax.named_scope("x_wait"):
                x_send(m, -1).wait_recv()

        x16 = dot(expand[...], xin[m])
        put_cols(cols_a, x16)
        z = conv(cols_a, w1) * gain + bias
        small = jnp.exp(-jnp.abs(4.0 * z))
        active = leak * z + (1.0 - leak) * (jnp.maximum(4.0 * z, 0.0) + jnp.log1p(small)) / 4.0
        put_cols(cols_b, jnp.where(keep, active, 0.0))
        share = jnp.where(z >= 0.0, 1.0, small) / (1.0 + small)
        slope[m] = jnp.where(keep, (leak + (1.0 - leak) * share) * gain, 0.0)
        y = (x16 + conv(cols_b, w2)).astype(bf16)

        @pl.when(section < sections - 1)
        def _():
            xsend[m] = dot(compact[...], y).astype(bf16)
            x_send(m).start()

        @pl.when(last)
        def _():
            pooled[pl.ds(0, 1), :] = jnp.sum(y.astype(f32) * dw16[...], axis=0, keepdims=True)

            @pl.when(m == 0)
            def _():
                embed_copy.wait()

            embedded = dot(pooled[...].astype(bf16), embed[...])[:1]
            square = jnp.mean(embedded * embedded, axis=-1, keepdims=True)
            factor = lax.rsqrt(square + tiny_value) / math.sqrt(width)
            normed = (embedded * factor).astype(bf16).astype(f32)
            emb[m] = embedded
            unit_src[m] = normed
            unit_all[m, me] = normed
            send_peers(0, m)

    def partial(m):
        with jax.named_scope("unit_wait"):
            recv_peers(0, m)
        for n in range(shards):
            flat[pl.ds(n, 1), :] = unit_all[m, n]
        cosines = dot_nt(flat[...].astype(bf16), centres[...])
        mine = pl.ds(pl.multiple_of(m * shards, shards), shards)
        logits = scale_value * (cosines - margin_value * hits[mine, :].astype(f32))
        grown = jnp.exp(logits)
        wide[:, pl.ds(0, width)] = dot(grown.astype(bf16), centres[...])
        wide[:, pl.ds(width, LANES)] = jnp.broadcast_to(
            jnp.sum(grown, axis=1, keepdims=True), (shards, LANES)
        )
        for n in range(shards):
            part_src[m, n] = wide[pl.ds(n, 1), :]
        part_rcv[m, me] = part_src[m, me]
        send_peers(2, m)

    def backward(m):
        @pl.when(last)
        def _():
            with jax.named_scope("chosen_wait"):
                recv_peers(1, m)
            chosen = jnp.sum(chosen_rcv[m], axis=0)
            with jax.named_scope("part_wait"):
                recv_peers(2, m)
            sums = jnp.sum(part_rcv[m], axis=0)
            grad_unit = scale_value * (sums[:, :width] / sums[:, width : width + 1] - chosen)
            embedded = emb[m]
            square = jnp.mean(embedded * embedded, axis=-1, keepdims=True)
            factor = lax.rsqrt(square + tiny_value) / math.sqrt(width)
            inner = jnp.sum(embedded * grad_unit, axis=-1, keepdims=True)
            grad_embed = factor * (
                grad_unit - embedded * inner / (width * (square + tiny_value))
            )
            gemb[pl.ds(0, 1), :] = grad_embed
            gpool = dot_nt(gemb[...].astype(bf16), embed[...])[:1]
            g16[...] = (gpool * dw16[...]).astype(bf16).astype(f32)

        @pl.when(section < sections - 1)
        def _():
            with jax.named_scope("g_wait"):
                g_send(m, 1).wait_recv()
            g16[...] = dot(expand[...], gin[m])

        put_cols(cols_a, g16[...])
        grad_hidden = conv(cols_a, w2t) * slope[m]
        put_cols(cols_b, grad_hidden)
        result = (g16[...] + conv(cols_b, w1t)).astype(bf16)
        gout[m] = dot(compact[...], result).astype(bf16)

        @pl.when(section > 0)
        def _():
            g_send(m).start()

        out_copy(m).start()

    def drain():
        @pl.loop(0, images)
        def _(m):
            @pl.when(section < sections - 1)
            def _():
                x_send(m).wait_send()

            @pl.when(section > 0)
            def _():
                g_send(m).wait_send()

            out_copy(m).wait()

        @pl.when(last)
        def _():
            @pl.loop(0, images)
            def _(m):
                for kind in range(3):
                    drain_peers(kind, m)

    lag = 4

    @pl.loop(0, images + lag)
    def _(t):
        @pl.when(t < images)
        def _():
            with jax.named_scope("forward"):
                forward(t)

        @pl.when((section < sections - 1) & (t == images - 1))
        def _():
            with jax.named_scope("flip"):
                flip(w2, w2t)
                flip(w1, w1t)

        @pl.when(last & (t >= 2) & (t < images + 2))
        def _():
            with jax.named_scope("partial"):
                partial(t - 2)

        @pl.when(t >= lag)
        def _():
            with jax.named_scope("backward"):
                backward(t - lag)

    with jax.named_scope("drain"):
        drain()


def on_device(
    section_input,
    conv_one,
    conv_two,
    unit_gain,
    offset_bias,
    leak_slope,
    depthwise,
    embed_weight,
    class_centers,
    labels,
    class_offsets,
):
    sections = lax.axis_size("section")
    shards = lax.axis_size("shard")
    micro, local, positions, channels = section_input.shape
    side = math.isqrt(positions)
    images = micro * local
    rows = side * STRIDE
    width = embed_weight.shape[1]
    classes = class_centers.shape[0]
    faces = shards * images
    vmem = pl.BlockSpec(memory_space=pltpu.VMEM)
    smem = pl.BlockSpec(memory_space=pltpu.SMEM)
    hbm = pl.BlockSpec(memory_space=pl.ANY)
    dma = pltpu.SemaphoreType.DMA
    maps = pltpu.VMEM((images, positions, channels), bf16)
    weights = pltpu.VMEM(conv_one.shape[1:], bf16)
    columns = pltpu.VMEM((rows + 2 * STRIDE, 3 * channels), bf16)
    result = pl.pallas_call(
        functools.partial(kernel, sections, shards, images, side),
        out_shape=jax.ShapeDtypeStruct((images, positions, channels), bf16),
        in_specs=[hbm, hbm, hbm, vmem, vmem, vmem, vmem, hbm, hbm, vmem, smem],
        out_specs=hbm,
        scratch_shapes=[
            pltpu.VMEM((positions, images, channels), bf16),
            maps,
            maps,
            maps,
            maps,
            weights,
            weights,
            weights,
            weights,
            pltpu.VMEM(embed_weight.shape, bf16),
            pltpu.VMEM((classes, width), bf16),
            pltpu.VMEM((classes, width), bf16),
            columns,
            columns,
            pltpu.VMEM((rows, positions), bf16),
            pltpu.VMEM((positions, rows), bf16),
            pltpu.VMEM((rows, channels), f32),
            pltpu.VMEM((images, rows, channels), f32),
            pltpu.VMEM((rows, channels), f32),
            pltpu.VMEM((HALF_ROWS, channels), f32),
            pltpu.VMEM((images, 1, width), f32),
            pltpu.VMEM((HALF_ROWS, width), f32),
            pltpu.VMEM((images, 1, width), f32),
            pltpu.VMEM((images, shards, 1, width), f32),
            pltpu.VMEM((shards, width), f32),
            pltpu.VMEM((shards, width + LANES), f32),
            pltpu.VMEM((faces, 1), f32),
            pltpu.VMEM((faces, classes), bf16),
            pltpu.VMEM((faces, width), f32),
            pltpu.VMEM((images, shards, 1, width), f32),
            pltpu.VMEM((images, shards, 1, width), f32),
            pltpu.VMEM((images, shards, 1, width + LANES), f32),
            pltpu.VMEM((images, shards, 1, width + LANES), f32),
            dma((4,)),
            dma((images,)),
            dma((images,)),
            dma((images,)),
            dma((images,)),
            dma((images,)),
            dma((images,)),
            dma((3, images)),
            dma((3, images)),
        ],
        compiler_params=pltpu.CompilerParams(
            collective_id=0, has_side_effects=True, vmem_limit_bytes=60000 * 1024
        ),
        name="window",
    )(
        section_input.transpose(2, 0, 1, 3).reshape(positions, images, channels),
        conv_one,
        conv_two,
        unit_gain,
        offset_bias,
        leak_slope,
        depthwise,
        embed_weight,
        class_centers,
        labels,
        class_offsets,
    )
    return result.reshape(1, micro, local, positions, channels)


def solution(mesh):
    placed = (
        P(None, "shard", None, None),
        P("section", None, None),
        P("section", None, None),
        P("section", None),
        P("section", None),
        P("section", None),
        P(),
        P(),
        P("shard", None),
        P(),
        P("shard"),
    )
    return jax.shard_map(
        on_device,
        mesh=mesh,
        in_specs=placed,
        out_specs=P("section", None, "shard", None, None),
        check_vma=False,
    )
```
